256 devices in a mesh: sta: 16 (over y, x), evt: 16 (over z, core).
Axes of the slice: x: 4, y: 4, z: 8, core: 2. Of those that a mesh axis runs over, the one named last changes fastest.
Arguments:
- traces: bfloat16 [3, 128, 1024, 2048], P(None, 'sta', 'evt'), may hold values from -96 to 96
- baz_bin: int32 [128, 1024], P('sta', 'evt'), may hold values from 0 to 35
- inc_bin: int32 [128, 1024], P('sta', 'evt'), may hold values from 0 to 7
- counts: int32 [128], P('sta'), may hold values from 128 to 1024
- depth_index: int32 [128, 512], P('sta'), may hold values from 0 to 2046
- tile_of: int32 [128], replicated, may hold values from 0 to 63
Outputs:
- stack: float32 [64, 5, 2, 512], P('sta', None, None, 'evt')
The draws below stay inside these ranges and needn't reach their ends.
All inputs are finite; a program needn't handle non-finite values.
Results may differ from the reference program's by a relative error of at most 0.0003.
Values sent between devices are 32-bit elements; how exact they have to be, the bound alone decides.
No kernel may reach another device: no remote copies, remote signals or barrier semaphores. Data moves between devices by JAX's collectives and lax.ppermute only.
A program may use at most 64 MiB of HBM per device.

```python
import jax
import jax.numpy as jnp
from jax import lax

NS = 2048
DEPTHS = 512
BAZ_BINS = 36
INC_BINS = 8
STATIONS = 128
EVENTS = 1024
TILES = 64


def set_ends(result, own_key, low, top_value):
    longest = result.shape.index(max(result.shape))
    spots = []
    for shift in (0, 1):
        where = [jax.random.randint(jax.random.fold_in(own_key, axis), (), 0, length) for axis, length in enumerate(result.shape)]
        where[longest] = (where[longest] + shift) % result.shape[longest]
        spots.append(tuple(where))
    return result.at[spots[0]].set(low).at[spots[1]].set(top_value)


def block_scale(stream_key, dims, shards, low, high):
    factor_of = 1.0
    for dim, parts in shards:
        steps = jax.random.uniform(jax.random.fold_in(jax.random.fold_in(stream_key, 6), dim), (parts,), jnp.float32, low / len(shards), high / len(shards))
        factor_of = factor_of * jnp.repeat(jnp.exp(steps), dims[dim] // parts).reshape((-1,) + (1,) * (len(dims) - 1 - dim))
    return factor_of


def centred(own_key, shape, deviation, bound, shards=(), kind=jnp.bfloat16):
    result = deviation * jax.random.normal(own_key, shape, jnp.float32)
    if shards:
        result = result * block_scale(own_key, shape, shards, -0.22, 0.18)
    return jnp.clip(result, -bound, bound).astype(kind)


def setup_inputs(seed: int = 0) -> dict:
    key_of = jax.random.split(jax.random.key(seed), 7)
    return {
        "traces": centred(key_of[0], (3, STATIONS, EVENTS, NS), 16.0, 96.0, ((1, 16), (2, 16))),
        "baz_bin": set_ends(jax.random.randint(key_of[1], (STATIONS, EVENTS), 0, BAZ_BINS), jax.random.fold_in(key_of[1], 1), 0, BAZ_BINS - 1).astype(jnp.int32),
        "inc_bin": set_ends(jax.random.randint(key_of[2], (STATIONS, EVENTS), 0, INC_BINS), jax.random.fold_in(key_of[2], 1), 0, INC_BINS - 1).astype(jnp.int32),
        "counts": set_ends(jax.random.randint(key_of[3], (STATIONS,), EVENTS // 8, EVENTS + 1), jax.random.fold_in(key_of[3], 1), EVENTS // 8, EVENTS).astype(jnp.int32),
        "depth_index": set_ends(jax.random.randint(key_of[4], (STATIONS, DEPTHS), 0, NS - 1), jax.random.fold_in(key_of[4], 1), 0, (NS - 1) - 1).astype(jnp.int32),
        "tile_of": set_ends(jax.random.randint(key_of[5], (STATIONS,), 0, TILES), jax.random.fold_in(key_of[5], 1), 0, TILES - 1).astype(jnp.int32),
    }


def reference(traces, baz_bin, inc_bin, counts, depth_index, tile_of):
    highest = lax.Precision.HIGHEST

    def one_station(station):
        block = lax.dynamic_index_in_dim(traces, station, 1, keepdims=False).astype(jnp.float32)
        bins = lax.dynamic_index_in_dim(baz_bin, station, 0, keepdims=False)
        tilts = lax.dynamic_index_in_dim(inc_bin, station, 0, keepdims=False)
        total = lax.dynamic_index_in_dim(counts, station, 0, keepdims=False)
        indices = lax.dynamic_index_in_dim(depth_index, station, 0, keepdims=False).astype(jnp.int32)
        phi = (bins.astype(jnp.float32) + 0.5) * (2.0 * jnp.pi / BAZ_BINS)
        incidence = (12.0 + 2.5 * (tilts.astype(jnp.float32) + 0.5)) * (jnp.pi / 180.0)
        cosine = jnp.cos(phi)[:, None]
        sine = jnp.sin(phi)[:, None]
        radial = -(cosine * block[1] + sine * block[2])
        quality = jnp.cos(incidence)[:, None] * radial + jnp.sin(incidence)[:, None] * block[0]
        transverse = sine * block[1] - cosine * block[2]
        data = jnp.concatenate([quality, transverse], axis=1)
        live = (jnp.arange(EVENTS) < total).astype(jnp.float32)
        harm = jnp.stack([jnp.ones_like(phi), jnp.cos(phi), jnp.sin(phi), jnp.cos(2.0 * phi), jnp.sin(2.0 * phi)], axis=1)
        weighted = harm * live[:, None]
        normal = jnp.dot(weighted.T, harm, precision=highest) + jnp.eye(5, dtype=jnp.float32)
        rhs = jnp.dot(weighted.T, data, precision=highest)
        coeff = jnp.linalg.solve(normal, rhs).reshape(5, 2, NS)
        return 0.5 * (coeff[:, :, indices] + coeff[:, :, indices + 1])
    profiles = lax.map(one_station, jnp.arange(STATIONS))
    onehot = (tile_of[None, :] == jnp.arange(TILES)[:, None]).astype(jnp.float32)
    sums = jnp.einsum('ts,skcz->tkcz', onehot, profiles, precision=highest)
    members = jnp.sum(onehot, axis=1)
    return sums / jnp.maximum(members, 1.0)[:, None, None, None]
```

```python
import jax
import jax.numpy as jnp
from jax import lax
from jax.experimental import pallas as pl
from jax.experimental.pallas import tpu as pltpu
from jax.sharding import PartitionSpec as P

NS = 2048
DEPTHS = 512
BAZ_BINS = 36
TILE_DEV = 4
STA = 8
EVT = 64
ROWS = 10
PAIRS = [(k, l) for k in range(5) for l in range(k, 5)]
CHUNKS = 4
WIDTH = NS // CHUNKS


def fit_kernel(traces, baz_ref, inc_ref, counts, depth_ref, out_ref, data, lhs, acc, sems):
    copies = []
    for n in range(CHUNKS):
        cols = pl.ds(n * WIDTH, WIDTH)
        copy = pltpu.make_async_copy(
            traces.at[:, :, :, cols], data.at[:, :, :, cols], sems.at[n]
        )
        copy.start()
        copies.append(copy)

    lane = lax.broadcasted_iota(jnp.int32, (STA, 128), 1)
    row = lax.broadcasted_iota(jnp.int32, (STA, 128), 0)
    baz = jnp.concatenate([baz_ref[...], baz_ref[...]], axis=1)
    inc = jnp.concatenate([inc_ref[...], inc_ref[...]], axis=1)
    phi = (baz.astype(jnp.float32) + 0.5) * (2.0 * jnp.pi / BAZ_BINS)
    tilt = (12.0 + 2.5 * (inc.astype(jnp.float32) + 0.5)) * (jnp.pi / 180.0)
    cosine = jnp.cos(phi)
    sine = jnp.sin(phi)
    cos_inc = jnp.cos(tilt)
    sin_inc = jnp.sin(tilt)
    total = jnp.zeros((STA, 128), jnp.int32)
    for s in range(STA):
        total = jnp.where(row == s, counts[s], total)
    slot = lax.axis_index("evt") * EVT + (lane & (EVT - 1))
    live = (slot < total).astype(jnp.float32)
    harm = [
        jnp.ones_like(phi),
        cosine,
        sine,
        1.0 - 2.0 * sine * sine,
        2.0 * sine * cosine,
    ]
    weighted = [h * live for h in harm]

    normal = jnp.zeros((STA, 128), jnp.float32)
    for i, (k, l) in enumerate(PAIRS):
        entry = jnp.where(lane < EVT, weighted[k] * harm[l], 0.0)
        normal = jnp.where(lane == 64 + i, jnp.sum(entry, axis=1, keepdims=True), normal)

    quality = [sin_inc, -cos_inc * cosine, -cos_inc * sine]
    transverse = [None, sine, -cosine]
    own = [((row >> 1) == v) & ((lane >> 6) == (row & 1)) for v in range(4)]
    for comp in range(3):
        for v in range(4):
            parts = []
            for split in range(2):
                for k in range(5):
                    for base in (quality[comp], transverse[comp]):
                        if base is None:
                            parts.append(jnp.zeros((STA, 128), jnp.float32))
                            continue
                        value = weighted[k] * base
                        high = value.astype(jnp.bfloat16).astype(jnp.float32)
                        piece = high if split == 0 else value - high
                        parts.append(jnp.where(own[v], piece, 0.0))
            block = jnp.concatenate(parts, axis=0).astype(jnp.bfloat16)
            lhs[:, pl.ds((comp * 4 + v) * 128, 128)] = block

    for n in range(CHUNKS):
        copies[n].wait()
        cols = pl.ds(n * WIDTH, WIDTH)
        block = data[:, :, :, cols].reshape(3 * STA * EVT, WIDTH)
        product = jnp.dot(lhs[...], block, preferred_element_type=jnp.float32)
        acc[:, cols] = product[: ROWS * STA] + product[ROWS * STA :]

    depth = depth_ref[...]
    rolled = []
    for b in range(4):
        piece = depth[:, b * 128 : (b + 1) * 128]
        for q in range(4):
            moved = pltpu.roll(piece, q * 32, 1) if q else piece
            rolled.append((moved >> 7, moved & 127))
    group = lane >> 5
    picked = {}
    for r in range(ROWS):
        q = r % 4
        strips = [acc[pl.ds(r * STA, STA), pl.ds(b * 128, 128)] for b in range(16)]
        turned = [pltpu.roll(strip, 127, 1) for strip in strips]
        means = []
        for b in range(16):
            after = turned[b] if b == 15 else jnp.where(lane == 127, turned[b + 1], turned[b])
            means.append(0.5 * (strips[b] + after))
        for b in range(4):
            high, low = rolled[b * 4 + q]
            result = jnp.take_along_axis(means[0], low, axis=1)
            for t in range(1, 16):
                result = jnp.where(high == t, jnp.take_along_axis(means[t], low, axis=1), result)
            picked[r, b] = result
    for b in range(4):
        for jj in range(4):
            for g in range(3):
                value = None
                for p in range(4):
                    r = 4 * g + (p - jj) % 4
                    if r >= ROWS:
                        if r > ROWS:
                            continue
                        source = pltpu.roll(normal, jj * 32, 1) if jj else normal
                        where = (group == p) | (group == (p + 1) % 4)
                    else:
                        source = picked[r, b]
                        where = group == p
                    value = source if value is None else jnp.where(where, source, value)
                out_ref[b * 4 + jj, pl.ds(g * 8, 8), :] = value


def solve_kernel(parts_ref, tile_ref, out_ref):
    lane = lax.broadcasted_iota(jnp.int32, (STA, 128), 1)
    total = jnp.sum(parts_ref[...], axis=0)
    back = lax.rem(4 - lax.rem(lax.axis_index("evt"), 4), 4) * 32
    mine = [pltpu.roll(total[g * 8 : (g + 1) * 8], back, 1) for g in range(3)]
    entry = {}
    for i, (k, l) in enumerate(PAIRS):
        value = jnp.broadcast_to(mine[2][:, 64 + i : 65 + i], (STA, 128))
        entry[k, l] = value + 1.0 if k == l else value
    right = []
    for k in range(5):
        right.append(pltpu.roll(mine[k // 2], 64, 1) if k % 2 else mine[k // 2])
    inverse = []
    for k in range(5):
        inv = 1.0 / entry[k, k]
        inverse.append(inv)
        for l in range(k + 1, 5):
            factor = entry[k, l] * inv
            for m in range(l, 5):
                entry[l, m] = entry[l, m] - factor * entry[k, m]
            right[l] = right[l] - factor * right[k]
    solved = [None] * 5
    for k in reversed(range(5)):
        value = right[k]
        for l in range(k + 1, 5):
            value = value - entry[k, l] * solved[l]
        solved[k] = value * inverse[k]
    low = lane < 64
    joined = jnp.concatenate(
        [
            jnp.where(low, solved[0], pltpu.roll(solved[1], 64, 1)),
            jnp.where(low, solved[2], pltpu.roll(solved[3], 64, 1)),
            jnp.where(low, solved[4], 0.0),
        ],
        axis=1,
    )
    shift = lax.rem(128 - lax.axis_index("sta") * STA, 128)
    local = pltpu.roll(jnp.broadcast_to(tile_ref[...], (8, 128)), shift, 1)[0:1, 0:STA]
    ids = lax.broadcasted_iota(jnp.int32, (64, STA), 0)
    onehot = (jnp.broadcast_to(local, (64, STA)) == ids).astype(jnp.float32)
    sums = jnp.dot(
        onehot, joined, precision=lax.Precision.HIGHEST, preferred_element_type=jnp.float32
    )
    for i in range(16):
        out_ref[i] = sums[i * TILE_DEV : (i + 1) * TILE_DEV]


def stack_kernel(parts_ref, tile_ref, out_ref):
    sums = jnp.sum(parts_ref[...], axis=0)
    own = lax.axis_index("sta") * TILE_DEV + lax.broadcasted_iota(jnp.int32, (TILE_DEV, 128), 0)
    match = (jnp.broadcast_to(tile_ref[...], (TILE_DEV, 128)) == own).astype(jnp.float32)
    members = jnp.sum(match, axis=1, keepdims=True)
    result = sums / jnp.maximum(members, 1.0)
    for k in range(5):
        for c in range(2):
            out_ref[:, k, c, :] = result[:, k * 64 + c * 32 : k * 64 + c * 32 + 32]


def body(traces, baz_bin, inc_bin, counts, depth_index, tile_of):
    vmem = pl.BlockSpec(memory_space=pltpu.VMEM)
    partial = pl.pallas_call(
        fit_kernel,
        out_shape=jax.ShapeDtypeStruct((16, 24, 128), jnp.float32),
        in_specs=[
            pl.BlockSpec(memory_space=pl.ANY),
            vmem,
            vmem,
            pl.BlockSpec(memory_space=pltpu.SMEM),
            vmem,
        ],
        out_specs=vmem,
        scratch_shapes=[
            pltpu.VMEM((3, STA, EVT, NS), jnp.bfloat16),
            pltpu.VMEM((2 * ROWS * STA, 3 * STA * EVT), jnp.bfloat16),
            pltpu.VMEM((ROWS * STA, NS), jnp.float32),
            pltpu.SemaphoreType.DMA((CHUNKS,)),
        ],
        name="fit",
    )(traces, baz_bin, inc_bin, counts, depth_index)
    arrived = lax.all_to_all(partial, "evt", 0, 0, tiled=True)
    tiles = tile_of.reshape(1, 128)
    sums = pl.pallas_call(
        solve_kernel,
        out_shape=jax.ShapeDtypeStruct((16, TILE_DEV, 384), jnp.float32),
        in_specs=[vmem, vmem],
        out_specs=vmem,
        name="solve",
    )(arrived, tiles)
    landed = lax.all_to_all(sums, "sta", 0, 0, tiled=True)
    return pl.pallas_call(
        stack_kernel,
        out_shape=jax.ShapeDtypeStruct((TILE_DEV, 5, 2, 32), jnp.float32),
        in_specs=[vmem, vmem],
        out_specs=vmem,
        name="stack",
    )(landed, tiles)


def solution(mesh):
    return jax.shard_map(
        body,
        mesh=mesh,
        in_specs=(
            P(None, "sta", "evt", None),
            P("sta", "evt"),
            P("sta", "evt"),
            P("sta"),
            P("sta", None),
            P(),
        ),
        out_specs=P("sta", None, None, "evt"),
        check_vma=False,
    )
```

```python
import jax
import jax.numpy as jnp
from jax import lax
from jax.experimental import pallas as pl
from jax.experimental.pallas import tpu as pltpu
from jax.sharding import PartitionSpec as P

NS = 2048
DEPTHS = 512
BAZ_BINS = 36
TILE_DEV = 4
STA = 8
EVT = 64
ROWS = 10
PAIRS = [(k, l) for k in range(5) for l in range(k, 5)]
CHUNKS = 4
WIDTH = NS // CHUNKS


def fit_kernel(
    traces, baz_bin, inc_bin, counts_in, depth_index, out_ref,
    data, lhs, acc, baz_ref, inc_ref, counts, depth_ref, sems,
):
    small = []
    for i, (source, target) in enumerate(
        ((baz_bin, baz_ref), (inc_bin, inc_ref), (counts_in, counts), (depth_index, depth_ref))
    ):
        copy = pltpu.make_async_copy(source, target, sems.at[CHUNKS + i])
        copy.start()
        small.append(copy)
    copies = []
    for n in range(CHUNKS):
        cols = pl.ds(n * WIDTH, WIDTH)
        copy = pltpu.make_async_copy(
            traces.at[:, :, :, cols], data.at[:, :, :, cols], sems.at[n]
        )
        copy.start()
        copies.append(copy)

    for copy in small:
        copy.wait()
    lane = lax.broadcasted_iota(jnp.int32, (STA, 128), 1)
    row = lax.broadcasted_iota(jnp.int32, (STA, 128), 0)
    baz = jnp.concatenate([baz_ref[...], baz_ref[...]], axis=1)
    inc = jnp.concatenate([inc_ref[...], inc_ref[...]], axis=1)
    phi = (baz.astype(jnp.float32) + 0.5) * (2.0 * jnp.pi / BAZ_BINS)
    tilt = (12.0 + 2.5 * (inc.astype(jnp.float32) + 0.5)) * (jnp.pi / 180.0)
    cosine = jnp.cos(phi)
    sine = jnp.sin(phi)
    cos_inc = jnp.cos(tilt)
    sin_inc = jnp.sin(tilt)
    total = jnp.zeros((STA, 128), jnp.int32)
    for s in range(STA):
        total = jnp.where(row == s, counts[s], total)
    slot = lax.axis_index("evt") * EVT + (lane & (EVT - 1))
    live = (slot < total).astype(jnp.float32)
    harm = [
        jnp.ones_like(phi),
        cosine,
        sine,
        1.0 - 2.0 * sine * sine,
        2.0 * sine * cosine,
    ]
    weighted = [h * live for h in harm]

    normal = jnp.zeros((STA, 128), jnp.float32)
    for i, (k, l) in enumerate(PAIRS):
        entry = jnp.where(lane < EVT, weighted[k] * harm[l], 0.0)
        normal = jnp.where(lane == 64 + i, jnp.sum(entry, axis=1, keepdims=True), normal)

    quality = [sin_inc, -cos_inc * cosine, -cos_inc * sine]
    transverse = [None, sine, -cosine]
    own = [((row >> 1) == v) & ((lane >> 6) == (row & 1)) for v in range(4)]
    for comp in range(3):
        for v in range(4):
            parts = []
            for split in range(2):
                for k in range(5):
                    for base in (quality[comp], transverse[comp]):
                        if base is None:
                            parts.append(jnp.zeros((STA, 128), jnp.float32))
                            continue
                        value = weighted[k] * base
                        high = value.astype(jnp.bfloat16).astype(jnp.float32)
                        piece = high if split == 0 else value - high
                        parts.append(jnp.where(own[v], piece, 0.0))
            block = jnp.concatenate(parts, axis=0).astype(jnp.bfloat16)
            lhs[:, pl.ds((comp * 4 + v) * 128, 128)] = block

    for n in range(CHUNKS):
        copies[n].wait()
        cols = pl.ds(n * WIDTH, WIDTH)
        block = data[:, :, :, cols].reshape(3 * STA * EVT, WIDTH)
        product = jnp.dot(lhs[...], block, preferred_element_type=jnp.float32)
        acc[:, cols] = product[: ROWS * STA] + product[ROWS * STA :]

    depth = depth_ref[...]
    rolled = []
    for b in range(4):
        piece = depth[:, b * 128 : (b + 1) * 128]
        for q in range(4):
            moved = pltpu.roll(piece, q * 32, 1) if q else piece
            rolled.append((moved >> 7, moved & 127))
    group = lane >> 5
    picked = {}
    for r in range(ROWS):
        q = r % 4
        strips = [acc[pl.ds(r * STA, STA), pl.ds(b * 128, 128)] for b in range(16)]
        turned = [pltpu.roll(strip, 127, 1) for strip in strips]
        means = []
        for b in range(16):
            after = turned[b] if b == 15 else jnp.where(lane == 127, turned[b + 1], turned[b])
            means.append(0.5 * (strips[b] + after))
        for b in range(4):
            high, low = rolled[b * 4 + q]
            result = jnp.take_along_axis(means[0], low, axis=1)
            for t in range(1, 16):
                result = jnp.where(high == t, jnp.take_along_axis(means[t], low, axis=1), result)
            picked[r, b] = result
    for b in range(4):
        for jj in range(4):
            for g in range(3):
                value = None
                for p in range(4):
                    r = 4 * g + (p - jj) % 4
                    if r >= ROWS:
                        if r > ROWS:
                            continue
                        source = pltpu.roll(normal, jj * 32, 1) if jj else normal
                        where = (group == p) | (group == (p + 1) % 4)
                    else:
                        source = picked[r, b]
                        where = group == p
                    value = source if value is None else jnp.where(where, source, value)
                out_ref[b * 4 + jj, pl.ds(g * 8, 8), :] = value


def solve_kernel(parts_ref, tile_ref, out_ref):
    lane = lax.broadcasted_iota(jnp.int32, (STA, 128), 1)
    total = jnp.sum(parts_ref[...], axis=0)
    back = lax.rem(4 - lax.rem(lax.axis_index("evt"), 4), 4) * 32
    mine = [pltpu.roll(total[g * 8 : (g + 1) * 8], back, 1) for g in range(3)]
    entry = {}
    for i, (k, l) in enumerate(PAIRS):
        value = jnp.broadcast_to(mine[2][:, 64 + i : 65 + i], (STA, 128))
        entry[k, l] = value + 1.0 if k == l else value
    right = []
    for k in range(5):
        right.append(pltpu.roll(mine[k // 2], 64, 1) if k % 2 else mine[k // 2])
    inverse = []
    for k in range(5):
        inv = 1.0 / entry[k, k]
        inverse.append(inv)
        for l in range(k + 1, 5):
            factor = entry[k, l] * inv
            for m in range(l, 5):
                entry[l, m] = entry[l, m] - factor * entry[k, m]
            right[l] = right[l] - factor * right[k]
    solved = [None] * 5
    for k in reversed(range(5)):
        value = right[k]
        for l in range(k + 1, 5):
            value = value - entry[k, l] * solved[l]
        solved[k] = value * inverse[k]
    low = lane < 64
    joined = jnp.concatenate(
        [
            jnp.where(low, solved[0], pltpu.roll(solved[1], 64, 1)),
            jnp.where(low, solved[2], pltpu.roll(solved[3], 64, 1)),
            jnp.where(low, solved[4], 0.0),
        ],
        axis=1,
    )
    shift = lax.rem(128 - lax.axis_index("sta") * STA, 128)
    local = pltpu.roll(jnp.broadcast_to(tile_ref[...], (8, 128)), shift, 1)[0:1, 0:STA]
    ids = lax.broadcasted_iota(jnp.int32, (64, STA), 0)
    onehot = (jnp.broadcast_to(local, (64, STA)) == ids).astype(jnp.float32)
    sums = jnp.dot(
        onehot, joined, precision=lax.Precision.HIGHEST, preferred_element_type=jnp.float32
    )
    for i in range(16):
        out_ref[i] = sums[i * TILE_DEV : (i + 1) * TILE_DEV]


def stack_kernel(parts_ref, tile_ref, out_ref):
    sums = jnp.sum(parts_ref[...], axis=0)
    own = lax.axis_index("sta") * TILE_DEV + lax.broadcasted_iota(jnp.int32, (TILE_DEV, 128), 0)
    match = (jnp.broadcast_to(tile_ref[...], (TILE_DEV, 128)) == own).astype(jnp.float32)
    members = jnp.sum(match, axis=1, keepdims=True)
    result = sums / jnp.maximum(members, 1.0)
    for k in range(5):
        for c in range(2):
            out_ref[:, k, c, :] = result[:, k * 64 + c * 32 : k * 64 + c * 32 + 32]


def body(traces, baz_bin, inc_bin, counts, depth_index, tile_of):
    vmem = pl.BlockSpec(memory_space=pltpu.VMEM)
    partial = pl.pallas_call(
        fit_kernel,
        out_shape=jax.ShapeDtypeStruct((16, 24, 128), jnp.float32),
        in_specs=[pl.BlockSpec(memory_space=pltpu.HBM)] * 5,
        out_specs=vmem,
        scratch_shapes=[
            pltpu.VMEM((3, STA, EVT, NS), jnp.bfloat16),
            pltpu.VMEM((2 * ROWS * STA, 3 * STA * EVT), jnp.bfloat16),
            pltpu.VMEM((ROWS * STA, NS), jnp.float32),
            pltpu.VMEM((STA, EVT), jnp.int32),
            pltpu.VMEM((STA, EVT), jnp.int32),
            pltpu.SMEM((STA,), jnp.int32),
            pltpu.VMEM((STA, DEPTHS), jnp.int32),
            pltpu.SemaphoreType.DMA((CHUNKS + 4,)),
        ],
        compiler_params=pltpu.CompilerParams(vmem_limit_bytes=16 << 20),
        name="fit",
    )(*(pltpu.with_memory_space_constraint(x, pltpu.HBM) for x in (traces, baz_bin, inc_bin, counts, depth_index)))
    arrived = lax.all_to_all(partial, "evt", 0, 0, tiled=True)
    tiles = tile_of.reshape(1, 128)
    sums = pl.pallas_call(
        solve_kernel,
        out_shape=jax.ShapeDtypeStruct((16, TILE_DEV, 384), jnp.float32),
        in_specs=[vmem, vmem],
        out_specs=vmem,
        compiler_params=pltpu.CompilerParams(vmem_limit_bytes=4 << 20),
        name="solve",
    )(arrived, tiles)
    landed = lax.all_to_all(sums, "sta", 0, 0, tiled=True)
    return pl.pallas_call(
        stack_kernel,
        out_shape=jax.ShapeDtypeStruct((TILE_DEV, 5, 2, 32), jnp.float32),
        in_specs=[vmem, vmem],
        out_specs=vmem,
        compiler_params=pltpu.CompilerParams(vmem_limit_bytes=4 << 20),
        name="stack",
    )(landed, tiles)


def solution(mesh):
    return jax.shard_map(
        body,
        mesh=mesh,
        in_specs=(
            P(None, "sta", "evt", None),
            P("sta", "evt"),
            P("sta", "evt"),
            P("sta"),
            P("sta", None),
            P(),
        ),
        out_specs=P("sta", None, None, "evt"),
        check_vma=False,
    )
```

```python
import jax
import jax.numpy as jnp
from jax import lax
from jax.experimental import pallas as pl
from jax.experimental.pallas import tpu as pltpu
from jax.sharding import PartitionSpec as P

NS = 2048
DEPTHS = 512
BAZ_BINS = 36
TILE_DEV = 4
STA = 8
EVT = 64
ROWS = 10
PAIRS = [(k, l) for k in range(5) for l in range(k, 5)]
WIDTHS = (512,)*4
STARTS = tuple(range(0,2048,512))
CHUNKS = len(WIDTHS)


def fit_kernel(
    traces, baz_bin, inc_bin, counts_in, depth_index, out_ref,
    data, lhs, acc, mean, picked, baz_ref, inc_ref, counts, depth_ref, sems,
):
    small = []
    for i, (source, target) in enumerate(
        ((baz_bin, baz_ref), (inc_bin, inc_ref), (counts_in, counts), (depth_index, depth_ref))
    ):
        copy = pltpu.make_async_copy(source, target, sems.at[CHUNKS + i])
        copy.start()
        small.append(copy)
    copies = []
    for n in range(CHUNKS):
        cols = pl.ds(STARTS[n], WIDTHS[n])
        copy = pltpu.make_async_copy(
            traces.at[:, :, :, cols], data.at[:, :, :, cols], sems.at[n]
        )
        copy.start()
        copies.append(copy)

    for copy in small:
        copy.wait()
    lane = lax.broadcasted_iota(jnp.int32, (STA, 128), 1)
    row = lax.broadcasted_iota(jnp.int32, (STA, 128), 0)
    baz = jnp.concatenate([baz_ref[...], baz_ref[...]], axis=1)
    inc = jnp.concatenate([inc_ref[...], inc_ref[...]], axis=1)
    phi = (baz.astype(jnp.float32) + 0.5) * (2.0 * jnp.pi / BAZ_BINS)
    tilt = (12.0 + 2.5 * (inc.astype(jnp.float32) + 0.5)) * (jnp.pi / 180.0)
    cosine = jnp.cos(phi)
    sine = jnp.sin(phi)
    cos_inc = jnp.cos(tilt)
    sin_inc = jnp.sin(tilt)
    total = jnp.zeros((STA, 128), jnp.int32)
    for s in range(STA):
        total = jnp.where(row == s, counts[s], total)
    slot = lax.axis_index("evt") * EVT + (lane & (EVT - 1))
    live = (slot < total).astype(jnp.float32)
    harm = [
        jnp.ones_like(phi),
        cosine,
        sine,
        1.0 - 2.0 * sine * sine,
        2.0 * sine * cosine,
    ]
    weighted = [h * live for h in harm]

    normal = jnp.zeros((STA, 128), jnp.float32)
    for i, (k, l) in enumerate(PAIRS):
        entry = jnp.where(lane < EVT, weighted[k] * harm[l], 0.0)
        normal = jnp.where(lane == 64 + i, jnp.sum(entry, axis=1, keepdims=True), normal)

    quality = [sin_inc, -cos_inc * cosine, -cos_inc * sine]
    transverse = [None, sine, -cosine]
    own = [((row >> 1) == v) & ((lane >> 6) == (row & 1)) for v in range(4)]
    for comp in range(3):
        for v in range(4):
            parts = []
            for split in range(2):
                for k in range(5):
                    for base in (quality[comp], transverse[comp]):
                        if base is None:
                            parts.append(jnp.zeros((STA, 128), jnp.float32))
                            continue
                        value = weighted[k] * base
                        high = value.astype(jnp.bfloat16).astype(jnp.float32)
                        piece = high if split == 0 else value - high
                        parts.append(jnp.where(own[v], piece, 0.0))
            block = jnp.concatenate(parts, axis=0).astype(jnp.bfloat16)
            lhs[:, pl.ds((comp * 4 + v) * 128, 128)] = block

    depth = depth_ref[...]

    def pick(first, last):
        means = []
        for r in range(ROWS):
            rows = pl.ds(r * STA, STA)
            strips = [acc[rows, pl.ds(t * 128, 128)] for t in range(first, min(last + 1, 16))]
            turned = [pltpu.roll(strip, 127, 1) for strip in strips]
            for t in range(last - first):
                after = turned[t]
                if t + 1 < len(turned):
                    after = jnp.where(lane == 127, turned[t + 1], after)
                mean[r, first + t] = 0.5 * (strips[t] + after)
        for b in range(4):
            piece = depth[:, b * 128 : (b + 1) * 128]
            high, low = piece >> 7, piece & 127
            for r in range(ROWS):
                result = picked[r * 4 + b] if first else jnp.zeros((STA, 128), jnp.float32)
                for t in range(first, last):
                    result = jnp.where(
                        high == t, jnp.take_along_axis(mean[r, t], low, axis=1), result
                    )
                picked[r * 4 + b] = result

    done = 0
    for n in range(CHUNKS):
        copies[n].wait()
        cols = pl.ds(STARTS[n], WIDTHS[n])
        block = data[:, :, :, cols].reshape(3 * STA * EVT, WIDTHS[n])
        product = jnp.dot(lhs[...], block, preferred_element_type=jnp.float32)
        acc[:, cols] = product[: ROWS * STA] + product[ROWS * STA :]
        ready = STARTS[n] // 128 - 1
        if ready > done:
            pick(done, ready)
            done = ready
    pick(done, 16)
    group = lane >> 5
    turned = {
        (r, b): pltpu.roll(picked[r * 4 + b], (r % 4) * 32, 1) if r % 4 else picked[r * 4 + b]
        for r in range(ROWS)
        for b in range(4)
    }
    for b in range(4):
        for jj in range(4):
            for g in range(3):
                value = None
                for p in range(4):
                    r = 4 * g + (p - jj) % 4
                    if r >= ROWS:
                        if r > ROWS:
                            continue
                        source = pltpu.roll(normal, jj * 32, 1) if jj else normal
                        where = (group == p) | (group == (p + 1) % 4)
                    else:
                        source = turned[r, b]
                        where = group == p
                    value = source if value is None else jnp.where(where, source, value)
                out_ref[b * 4 + jj, pl.ds(g * 8, 8), :] = value


def solve_kernel(parts_ref, tile_ref, out_ref):
    lane = lax.broadcasted_iota(jnp.int32, (STA, 128), 1)
    total = jnp.sum(parts_ref[...], axis=0)
    back = lax.rem(4 - lax.rem(lax.axis_index("evt"), 4), 4) * 32
    mine = [pltpu.roll(total[g * 8 : (g + 1) * 8], back, 1) for g in range(3)]
    entry = {}
    for i, (k, l) in enumerate(PAIRS):
        value = jnp.broadcast_to(mine[2][:, 64 + i : 65 + i], (STA, 128))
        entry[k, l] = value + 1.0 if k == l else value
    right = []
    for k in range(5):
        right.append(pltpu.roll(mine[k // 2], 64, 1) if k % 2 else mine[k // 2])
    inverse = []
    for k in range(5):
        inv = 1.0 / entry[k, k]
        inverse.append(inv)
        for l in range(k + 1, 5):
            factor = entry[k, l] * inv
            for m in range(l, 5):
                entry[l, m] = entry[l, m] - factor * entry[k, m]
            right[l] = right[l] - factor * right[k]
    solved = [None] * 5
    for k in reversed(range(5)):
        value = right[k]
        for l in range(k + 1, 5):
            value = value - entry[k, l] * solved[l]
        solved[k] = value * inverse[k]
    low = lane < 64
    joined = jnp.concatenate(
        [
            jnp.where(low, solved[0], pltpu.roll(solved[1], 64, 1)),
            jnp.where(low, solved[2], pltpu.roll(solved[3], 64, 1)),
            jnp.where(low, solved[4], 0.0),
        ],
        axis=1,
    )
    shift = lax.rem(128 - lax.axis_index("sta") * STA, 128)
    local = pltpu.roll(jnp.broadcast_to(tile_ref[...], (8, 128)), shift, 1)[0:1, 0:STA]
    ids = lax.broadcasted_iota(jnp.int32, (64, STA), 0)
    onehot = (jnp.broadcast_to(local, (64, STA)) == ids).astype(jnp.float32)
    sums = jnp.dot(
        onehot, joined, precision=lax.Precision.HIGHEST, preferred_element_type=jnp.float32
    )
    for i in range(16):
        out_ref[i] = sums[i * TILE_DEV : (i + 1) * TILE_DEV]


def stack_kernel(parts_ref, tile_ref, out_ref):
    sums = jnp.sum(parts_ref[...], axis=0)
    own = lax.axis_index("sta") * TILE_DEV + lax.broadcasted_iota(jnp.int32, (TILE_DEV, 128), 0)
    match = (jnp.broadcast_to(tile_ref[...], (TILE_DEV, 128)) == own).astype(jnp.float32)
    members = jnp.sum(match, axis=1, keepdims=True)
    result = sums / jnp.maximum(members, 1.0)
    for k in range(5):
        for c in range(2):
            out_ref[:, k, c, :] = result[:, k * 64 + c * 32 : k * 64 + c * 32 + 32]


def body(traces, baz_bin, inc_bin, counts, depth_index, tile_of):
    vmem = pl.BlockSpec(memory_space=pltpu.VMEM)
    partial = pl.pallas_call(
        fit_kernel,
        out_shape=jax.ShapeDtypeStruct((16, 24, 128), jnp.float32),
        in_specs=[pl.BlockSpec(memory_space=pltpu.HBM)] * 5,
        out_specs=vmem,
        scratch_shapes=[
            pltpu.VMEM((3, STA, EVT, NS), jnp.bfloat16),
            pltpu.VMEM((2 * ROWS * STA, 3 * STA * EVT), jnp.bfloat16),
            pltpu.VMEM((ROWS * STA, NS), jnp.float32),
            pltpu.VMEM((ROWS, 16, STA, 128), jnp.float32),
            pltpu.VMEM((ROWS * 4, STA, 128), jnp.float32),
            pltpu.VMEM((STA, EVT), jnp.int32),
            pltpu.VMEM((STA, EVT), jnp.int32),
            pltpu.SMEM((STA,), jnp.int32),
            pltpu.VMEM((STA, DEPTHS), jnp.int32),
            pltpu.SemaphoreType.DMA((CHUNKS + 4,)),
        ],
        compiler_params=pltpu.CompilerParams(vmem_limit_bytes=16 << 20),
        name="fit",
    )(*(pltpu.with_memory_space_constraint(x, pltpu.HBM) for x in (traces, baz_bin, inc_bin, counts, depth_index)))
    arrived = lax.all_to_all(partial, "evt", 0, 0, tiled=True)
    tiles = tile_of.reshape(1, 128)
    sums = pl.pallas_call(
        solve_kernel,
        out_shape=jax.ShapeDtypeStruct((16, TILE_DEV, 384), jnp.float32),
        in_specs=[vmem, vmem],
        out_specs=vmem,
        compiler_params=pltpu.CompilerParams(vmem_limit_bytes=4 << 20),
        name="solve",
    )(arrived, tiles)
    landed = lax.all_to_all(sums, "sta", 0, 0, tiled=True)
    return pl.pallas_call(
        stack_kernel,
        out_shape=jax.ShapeDtypeStruct((TILE_DEV, 5, 2, 32), jnp.float32),
        in_specs=[vmem, vmem],
        out_specs=vmem,
        compiler_params=pltpu.CompilerParams(vmem_limit_bytes=4 << 20),
        name="stack",
    )(landed, tiles)


def solution(mesh):
    return jax.shard_map(
        body,
        mesh=mesh,
        in_specs=(
            P(None, "sta", "evt", None),
            P("sta", "evt"),
            P("sta", "evt"),
            P("sta"),
            P("sta", None),
            P(),
        ),
        out_specs=P("sta", None, None, "evt"),
        check_vma=False,
    )
```

```python
import jax
import jax.numpy as jnp
from jax import lax
from jax.experimental import pallas as pl
from jax.experimental.pallas import tpu as pltpu
from jax.sharding import PartitionSpec as P

NS = 2048
DEPTHS = 512
BAZ_BINS = 36
TILE_DEV = 4
EVT_ORDER = [(i + 11) % 16 for i in range(16)]
STA_ORDER = [(i + 10) % 16 for i in range(16)]
STA = 8
EVT = 64
ROWS = 10
PAIRS = [(k, l) for k in range(5) for l in range(k, 5)]
WIDTHS = (512,)*4
STARTS = tuple(range(0,2048,512))
CHUNKS = len(WIDTHS)


def fit_kernel(
    traces, baz_bin, inc_bin, counts_in, depth_index, out_ref,
    data, lhs, acc, mean, picked, baz_ref, inc_ref, counts, depth_ref, sems,
):
    small = []
    for i, (source, target) in enumerate(
        ((baz_bin, baz_ref), (inc_bin, inc_ref), (counts_in, counts), (depth_index, depth_ref))
    ):
        copy = pltpu.make_async_copy(source, target, sems.at[CHUNKS + i])
        copy.start()
        small.append(copy)
    copies = []
    for n in range(CHUNKS):
        cols = pl.ds(STARTS[n], WIDTHS[n])
        copy = pltpu.make_async_copy(
            traces.at[:, :, :, cols], data.at[:, :, :, cols], sems.at[n]
        )
        copy.start()
        copies.append(copy)

    for copy in small:
        copy.wait()
    lane = lax.broadcasted_iota(jnp.int32, (STA, 128), 1)
    row = lax.broadcasted_iota(jnp.int32, (STA, 128), 0)
    baz = jnp.concatenate([baz_ref[...], baz_ref[...]], axis=1)
    inc = jnp.concatenate([inc_ref[...], inc_ref[...]], axis=1)
    phi = (baz.astype(jnp.float32) + 0.5) * (2.0 * jnp.pi / BAZ_BINS)
    tilt = (12.0 + 2.5 * (inc.astype(jnp.float32) + 0.5)) * (jnp.pi / 180.0)
    cosine = jnp.cos(phi)
    sine = jnp.sin(phi)
    cos_inc = jnp.cos(tilt)
    sin_inc = jnp.sin(tilt)
    total = jnp.zeros((STA, 128), jnp.int32)
    for s in range(STA):
        total = jnp.where(row == s, counts[s], total)
    slot = lax.axis_index("evt") * EVT + (lane & (EVT - 1))
    live = (slot < total).astype(jnp.float32)
    harm = [
        jnp.ones_like(phi),
        cosine,
        sine,
        1.0 - 2.0 * sine * sine,
        2.0 * sine * cosine,
    ]
    weighted = [h * live for h in harm]

    normal = jnp.zeros((STA, 128), jnp.float32)
    for i, (k, l) in enumerate(PAIRS):
        entry = jnp.where(lane < EVT, weighted[k] * harm[l], 0.0)
        normal = jnp.where(lane == 64 + i, jnp.sum(entry, axis=1, keepdims=True), normal)

    quality = [sin_inc, -cos_inc * cosine, -cos_inc * sine]
    transverse = [None, sine, -cosine]
    own = [((row >> 1) == v) & ((lane >> 6) == (row & 1)) for v in range(4)]
    for comp in range(3):
        for v in range(4):
            parts = []
            for split in range(2):
                for k in range(5):
                    for base in (quality[comp], transverse[comp]):
                        if base is None:
                            parts.append(jnp.zeros((STA, 128), jnp.float32))
                            continue
                        value = weighted[k] * base
                        high = value.astype(jnp.bfloat16).astype(jnp.float32)
                        piece = high if split == 0 else value - high
                        parts.append(jnp.where(own[v], piece, 0.0))
            block = jnp.concatenate(parts, axis=0).astype(jnp.bfloat16)
            lhs[:, pl.ds((comp * 4 + v) * 128, 128)] = block

    depth = depth_ref[...]

    def pick(first, last):
        means = []
        for r in range(ROWS):
            rows = pl.ds(r * STA, STA)
            strips = [acc[rows, pl.ds(t * 128, 128)] for t in range(first, min(last + 1, 16))]
            turned = [pltpu.roll(strip, 127, 1) for strip in strips]
            for t in range(last - first):
                after = turned[t]
                if t + 1 < len(turned):
                    after = jnp.where(lane == 127, turned[t + 1], after)
                mean[r, first + t] = 0.5 * (strips[t] + after)
        for b in range(4):
            piece = depth[:, b * 128 : (b + 1) * 128]
            high, low = piece >> 7, piece & 127
            for r in range(ROWS):
                result = picked[r * 4 + b] if first else jnp.zeros((STA, 128), jnp.float32)
                for t in range(first, last):
                    result = jnp.where(
                        high == t, jnp.take_along_axis(mean[r, t], low, axis=1), result
                    )
                picked[r * 4 + b] = result

    done = 0
    for n in range(CHUNKS):
        copies[n].wait()
        cols = pl.ds(STARTS[n], WIDTHS[n])
        block = data[:, :, :, cols].reshape(3 * STA * EVT, WIDTHS[n])
        product = jnp.dot(lhs[...], block, preferred_element_type=jnp.float32)
        acc[:, cols] = product[: ROWS * STA] + product[ROWS * STA :]
        ready = STARTS[n] // 128 - 1
        if ready > done:
            pick(done, ready)
            done = ready
    pick(done, 16)
    group = lane >> 5
    turned = {
        (r, b): pltpu.roll(picked[r * 4 + b], (r % 4) * 32, 1) if r % 4 else picked[r * 4 + b]
        for r in range(ROWS)
        for b in range(4)
    }
    for b in range(4):
        for jj in range(4):
            for g in range(3):
                value = None
                for p in range(4):
                    r = 4 * g + (p - jj) % 4
                    if r >= ROWS:
                        if r > ROWS:
                            continue
                        source = pltpu.roll(normal, jj * 32, 1) if jj else normal
                        where = (group == p) | (group == (p + 1) % 4)
                    else:
                        source = turned[r, b]
                        where = group == p
                    value = source if value is None else jnp.where(where, source, value)
                out_ref[EVT_ORDER.index(b * 4 + jj), pl.ds(g * 8, 8), :] = value


def solve_kernel(parts_ref, tile_ref, out_ref):
    lane = lax.broadcasted_iota(jnp.int32, (STA, 128), 1)
    total = jnp.sum(parts_ref[...], axis=0)
    back = lax.rem(4 - lax.rem(lax.axis_index("evt"), 4), 4) * 32
    mine = [pltpu.roll(total[g * 8 : (g + 1) * 8], back, 1) for g in range(3)]
    entry = {}
    for i, (k, l) in enumerate(PAIRS):
        value = jnp.broadcast_to(mine[2][:, 64 + i : 65 + i], (STA, 128))
        entry[k, l] = value + 1.0 if k == l else value
    right = []
    for k in range(5):
        right.append(pltpu.roll(mine[k // 2], 64, 1) if k % 2 else mine[k // 2])
    inverse = []
    for k in range(5):
        inv = 1.0 / entry[k, k]
        inverse.append(inv)
        for l in range(k + 1, 5):
            factor = entry[k, l] * inv
            for m in range(l, 5):
                entry[l, m] = entry[l, m] - factor * entry[k, m]
            right[l] = right[l] - factor * right[k]
    solved = [None] * 5
    for k in reversed(range(5)):
        value = right[k]
        for l in range(k + 1, 5):
            value = value - entry[k, l] * solved[l]
        solved[k] = value * inverse[k]
    low = lane < 64
    joined = jnp.concatenate(
        [
            jnp.where(low, solved[0], pltpu.roll(solved[1], 64, 1)),
            jnp.where(low, solved[2], pltpu.roll(solved[3], 64, 1)),
            jnp.where(low, solved[4], 0.0),
        ],
        axis=1,
    )
    shift = lax.rem(128 - lax.axis_index("sta") * STA, 128)
    local = pltpu.roll(jnp.broadcast_to(tile_ref[...], (8, 128)), shift, 1)[0:1, 0:STA]
    ids = lax.broadcasted_iota(jnp.int32, (64, STA), 0)
    onehot = (jnp.broadcast_to(local, (64, STA)) == ids).astype(jnp.float32)
    sums = jnp.dot(
        onehot, joined, precision=lax.Precision.HIGHEST, preferred_element_type=jnp.float32
    )
    for i in range(16):
        out_ref[STA_ORDER.index(i)] = sums[i * TILE_DEV : (i + 1) * TILE_DEV]


def stack_kernel(parts_ref, tile_ref, out_ref):
    sums = jnp.sum(parts_ref[...], axis=0)
    own = lax.axis_index("sta") * TILE_DEV + lax.broadcasted_iota(jnp.int32, (TILE_DEV, 128), 0)
    match = (jnp.broadcast_to(tile_ref[...], (TILE_DEV, 128)) == own).astype(jnp.float32)
    members = jnp.sum(match, axis=1, keepdims=True)
    result = sums / jnp.maximum(members, 1.0)
    for k in range(5):
        for c in range(2):
            out_ref[:, k, c, :] = result[:, k * 64 + c * 32 : k * 64 + c * 32 + 32]


def body(traces, baz_bin, inc_bin, counts, depth_index, tile_of):
    vmem = pl.BlockSpec(memory_space=pltpu.VMEM)
    partial = pl.pallas_call(
        fit_kernel,
        out_shape=jax.ShapeDtypeStruct((16, 24, 128), jnp.float32),
        in_specs=[pl.BlockSpec(memory_space=pltpu.HBM)] * 5,
        out_specs=vmem,
        scratch_shapes=[
            pltpu.VMEM((3, STA, EVT, NS), jnp.bfloat16),
            pltpu.VMEM((2 * ROWS * STA, 3 * STA * EVT), jnp.bfloat16),
            pltpu.VMEM((ROWS * STA, NS), jnp.float32),
            pltpu.VMEM((ROWS, 16, STA, 128), jnp.float32),
            pltpu.VMEM((ROWS * 4, STA, 128), jnp.float32),
            pltpu.VMEM((STA, EVT), jnp.int32),
            pltpu.VMEM((STA, EVT), jnp.int32),
            pltpu.SMEM((STA,), jnp.int32),
            pltpu.VMEM((STA, DEPTHS), jnp.int32),
            pltpu.SemaphoreType.DMA((CHUNKS + 4,)),
        ],
        compiler_params=pltpu.CompilerParams(vmem_limit_bytes=16 << 20),
        name="fit",
    )(*(pltpu.with_memory_space_constraint(x, pltpu.HBM) for x in (traces, baz_bin, inc_bin, counts, depth_index)))
    arrived = lax.all_to_all(partial, "evt", 0, 0, tiled=True, axis_index_groups=[EVT_ORDER])
    tiles = tile_of.reshape(1, 128)
    sums = pl.pallas_call(
        solve_kernel,
        out_shape=jax.ShapeDtypeStruct((16, TILE_DEV, 384), jnp.float32),
        in_specs=[vmem, vmem],
        out_specs=vmem,
        compiler_params=pltpu.CompilerParams(vmem_limit_bytes=4 << 20),
        name="solve",
    )(arrived, tiles)
    landed = lax.all_to_all(sums, "sta", 0, 0, tiled=True, axis_index_groups=[STA_ORDER])
    return pl.pallas_call(
        stack_kernel,
        out_shape=jax.ShapeDtypeStruct((TILE_DEV, 5, 2, 32), jnp.float32),
        in_specs=[vmem, vmem],
        out_specs=vmem,
        compiler_params=pltpu.CompilerParams(vmem_limit_bytes=4 << 20),
        name="stack",
    )(landed, tiles)


def solution(mesh):
    return jax.shard_map(
        body,
        mesh=mesh,
        in_specs=(
            P(None, "sta", "evt", None),
            P("sta", "evt"),
            P("sta", "evt"),
            P("sta"),
            P("sta", None),
            P(),
        ),
        out_specs=P("sta", None, None, "evt"),
        check_vma=False,
    )
```

```python
import jax
import jax.numpy as jnp
from jax import lax
from jax.experimental import pallas as pl
from jax.experimental.pallas import tpu as pltpu
from jax.sharding import PartitionSpec as P

NS = 2048
DEPTHS = 512
BAZ_BINS = 36
TILE_DEV = 4
EVT_ORDER = [(i + 11) % 16 for i in range(16)]
STA_ORDER = [(i + 10) % 16 for i in range(16)]
STA = 8
EVT = 64
ROWS = 10
SHARE = 21
PAIRS = [(k, l) for k in range(5) for l in range(k, 5)]
WIDTHS = (512,)*4
STARTS = tuple(range(0,2048,512))
CHUNKS = len(WIDTHS)


def fit_kernel(
    traces, baz_bin, inc_bin, counts_in, depth_index, out_ref,
    data, lhs, acc, mean, picked, baz_ref, inc_ref, counts, depth_ref, sems,
):
    small = []
    for i, (source, target) in enumerate(
        ((baz_bin, baz_ref), (inc_bin, inc_ref), (counts_in, counts), (depth_index, depth_ref))
    ):
        copy = pltpu.make_async_copy(source, target, sems.at[CHUNKS + i])
        copy.start()
        small.append(copy)
    copies = []
    for n in range(CHUNKS):
        cols = pl.ds(STARTS[n], WIDTHS[n])
        copy = pltpu.make_async_copy(
            traces.at[:, :, :, cols], data.at[:, :, :, cols], sems.at[n]
        )
        copy.start()
        copies.append(copy)

    for copy in small:
        copy.wait()
    lane = lax.broadcasted_iota(jnp.int32, (STA, 128), 1)
    row = lax.broadcasted_iota(jnp.int32, (STA, 128), 0)
    baz = jnp.concatenate([baz_ref[...], baz_ref[...]], axis=1)
    inc = jnp.concatenate([inc_ref[...], inc_ref[...]], axis=1)
    phi = (baz.astype(jnp.float32) + 0.5) * (2.0 * jnp.pi / BAZ_BINS)
    tilt = (12.0 + 2.5 * (inc.astype(jnp.float32) + 0.5)) * (jnp.pi / 180.0)
    cosine = jnp.cos(phi)
    sine = jnp.sin(phi)
    cos_inc = jnp.cos(tilt)
    sin_inc = jnp.sin(tilt)
    total = jnp.zeros((STA, 128), jnp.int32)
    for s in range(STA):
        total = jnp.where(row == s, counts[s], total)
    slot = lax.axis_index("evt") * EVT + (lane & (EVT - 1))
    live = (slot < total).astype(jnp.float32)
    harm = [
        jnp.ones_like(phi),
        cosine,
        sine,
        1.0 - 2.0 * sine * sine,
        2.0 * sine * cosine,
    ]
    weighted = [h * live for h in harm]

    normal = jnp.zeros((STA, 128), jnp.float32)
    for i, (k, l) in enumerate(PAIRS):
        entry = jnp.where(lane < EVT, weighted[k] * harm[l], 0.0)
        normal = jnp.where(
            lane == row * 16 + i, jnp.sum(entry, axis=1, keepdims=True), normal
        )
    normal = jnp.sum(normal, axis=0, keepdims=True)

    quality = [sin_inc, -cos_inc * cosine, -cos_inc * sine]
    transverse = [None, sine, -cosine]
    own = [((row >> 1) == v) & ((lane >> 6) == (row & 1)) for v in range(4)]
    for comp in range(3):
        for v in range(4):
            parts = []
            for split in range(2):
                for k in range(5):
                    for base in (quality[comp], transverse[comp]):
                        if base is None:
                            parts.append(jnp.zeros((STA, 128), jnp.float32))
                            continue
                        value = weighted[k] * base
                        high = value.astype(jnp.bfloat16).astype(jnp.float32)
                        piece = high if split == 0 else value - high
                        parts.append(jnp.where(own[v], piece, 0.0))
            block = jnp.concatenate(parts, axis=0).astype(jnp.bfloat16)
            lhs[:, pl.ds((comp * 4 + v) * 128, 128)] = block

    depth = depth_ref[...]

    def pick(first, last):
        means = []
        for r in range(ROWS):
            rows = pl.ds(r * STA, STA)
            strips = [acc[rows, pl.ds(t * 128, 128)] for t in range(first, min(last + 1, 16))]
            turned = [pltpu.roll(strip, 127, 1) for strip in strips]
            for t in range(last - first):
                after = turned[t]
                if t + 1 < len(turned):
                    after = jnp.where(lane == 127, turned[t + 1], after)
                mean[r, first + t] = 0.5 * (strips[t] + after)
        for b in range(4):
            piece = depth[:, b * 128 : (b + 1) * 128]
            high, low = piece >> 7, piece & 127
            for r in range(ROWS):
                result = picked[r * 4 + b] if first else jnp.zeros((STA, 128), jnp.float32)
                for t in range(first, last):
                    result = jnp.where(
                        high == t, jnp.take_along_axis(mean[r, t], low, axis=1), result
                    )
                picked[r * 4 + b] = result

    done = 0
    for n in range(CHUNKS):
        copies[n].wait()
        cols = pl.ds(STARTS[n], WIDTHS[n])
        block = data[:, :, :, cols].reshape(3 * STA * EVT, WIDTHS[n])
        product = jnp.dot(lhs[...], block, preferred_element_type=jnp.float32)
        acc[:, cols] = product[: ROWS * STA] + product[ROWS * STA :]
        ready = STARTS[n] // 128 - 1
        if ready > done:
            pick(done, ready)
            done = ready
    pick(done, 16)
    group = lane >> 5
    turned = {}
    for r in range(ROWS):
        for b in range(4):
            whole = picked[r * 4 + b]
            turned[r, b] = pltpu.roll(whole, (r % 4) * 32, 1) if r % 4 else whole
            if r >= 8:
                turned[r + 2, b] = pltpu.roll(pltpu.roll(whole, 4, 0), (r % 4) * 32 + 64, 1)
    for b in range(4):
        for jj in range(4):
            base = EVT_ORDER.index(b * 4 + jj) * SHARE
            for g in range(3):
                value = turned[4 * g + (3 - jj) % 4, b]
                for p in range(3):
                    value = jnp.where(group == p, turned[4 * g + (p - jj) % 4, b], value)
                if g < 2:
                    out_ref[pl.ds(base + g * 8, 8), :] = value
                else:
                    out_ref[pl.ds(base + 16, 4), :] = value[0:4]
            out_ref[pl.ds(base + 20, 1), :] = normal


def solve_kernel(parts_ref, tile_ref, out_ref):
    lane = lax.broadcasted_iota(jnp.int32, (STA, 128), 1)
    row = lax.broadcasted_iota(jnp.int32, (STA, 128), 0)
    total = []
    for start, size in ((0, 8), (8, 8), (16, 5)):
        pieces = [parts_ref[pl.ds(j * SHARE + start, size), :] for j in range(16)]
        while len(pieces) > 1:
            pieces = [x + y for x, y in zip(pieces[::2], pieces[1::2])]
        total.append(pieces[0])
    normal = jnp.broadcast_to(total[2][4:5], (STA, 128))
    normal = jnp.take_along_axis(normal, row * 16 + (lane & 15), axis=1)
    back = lax.rem(4 - lax.rem(lax.axis_index("evt"), 4), 4) * 32
    folded = pltpu.roll(total[2][0:4], back, 1)
    mine = [
        pltpu.roll(total[0], back, 1),
        pltpu.roll(total[1], back, 1),
        jnp.concatenate([folded, pltpu.roll(folded, 64, 1)], axis=0),
    ]
    entry = {}
    for i, (k, l) in enumerate(PAIRS):
        value = jnp.broadcast_to(normal[:, i : i + 1], (STA, 128))
        entry[k, l] = value + 1.0 if k == l else value
    right = []
    for k in range(5):
        right.append(pltpu.roll(mine[k // 2], 64, 1) if k % 2 else mine[k // 2])
    inverse = []
    for k in range(5):
        inv = 1.0 / entry[k, k]
        inverse.append(inv)
        for l in range(k + 1, 5):
            factor = entry[k, l] * inv
            for m in range(l, 5):
                entry[l, m] = entry[l, m] - factor * entry[k, m]
            right[l] = right[l] - factor * right[k]
    solved = [None] * 5
    for k in reversed(range(5)):
        value = right[k]
        for l in range(k + 1, 5):
            value = value - entry[k, l] * solved[l]
        solved[k] = value * inverse[k]
    low = lane < 64
    joined = jnp.concatenate(
        [
            jnp.where(low, solved[0], pltpu.roll(solved[1], 64, 1)),
            jnp.where(low, solved[2], pltpu.roll(solved[3], 64, 1)),
            jnp.where(low, solved[4], 0.0),
        ],
        axis=1,
    )
    shift = lax.rem(128 - lax.axis_index("sta") * STA, 128)
    local = pltpu.roll(jnp.broadcast_to(tile_ref[...], (8, 128)), shift, 1)[0:1, 0:STA]
    ids = lax.broadcasted_iota(jnp.int32, (64, STA), 0)
    onehot = (jnp.broadcast_to(local, (64, STA)) == ids).astype(jnp.float32)
    sums = jnp.dot(
        onehot, joined, precision=lax.Precision.HIGHEST, preferred_element_type=jnp.float32
    )
    for i in range(16):
        out_ref[STA_ORDER.index(i)] = sums[i * TILE_DEV : (i + 1) * TILE_DEV]


def stack_kernel(parts_ref, tile_ref, out_ref):
    sums = jnp.sum(parts_ref[...], axis=0)
    own = lax.axis_index("sta") * TILE_DEV + lax.broadcasted_iota(jnp.int32, (TILE_DEV, 128), 0)
    match = (jnp.broadcast_to(tile_ref[...], (TILE_DEV, 128)) == own).astype(jnp.float32)
    members = jnp.sum(match, axis=1, keepdims=True)
    result = sums / jnp.maximum(members, 1.0)
    for k in range(5):
        for c in range(2):
            out_ref[:, k, c, :] = result[:, k * 64 + c * 32 : k * 64 + c * 32 + 32]


def body(traces, baz_bin, inc_bin, counts, depth_index, tile_of):
    vmem = pl.BlockSpec(memory_space=pltpu.VMEM)
    partial = pl.pallas_call(
        fit_kernel,
        out_shape=jax.ShapeDtypeStruct((16 * SHARE, 128), jnp.float32),
        in_specs=[pl.BlockSpec(memory_space=pltpu.HBM)] * 5,
        out_specs=vmem,
        scratch_shapes=[
            pltpu.VMEM((3, STA, EVT, NS), jnp.bfloat16),
            pltpu.VMEM((2 * ROWS * STA, 3 * STA * EVT), jnp.bfloat16),
            pltpu.VMEM((ROWS * STA, NS), jnp.float32),
            pltpu.VMEM((ROWS, 16, STA, 128), jnp.float32),
            pltpu.VMEM((ROWS * 4, STA, 128), jnp.float32),
            pltpu.VMEM((STA, EVT), jnp.int32),
            pltpu.VMEM((STA, EVT), jnp.int32),
            pltpu.SMEM((STA,), jnp.int32),
            pltpu.VMEM((STA, DEPTHS), jnp.int32),
            pltpu.SemaphoreType.DMA((CHUNKS + 4,)),
        ],
        compiler_params=pltpu.CompilerParams(vmem_limit_bytes=16 << 20),
        name="fit",
    )(*(pltpu.with_memory_space_constraint(x, pltpu.HBM) for x in (traces, baz_bin, inc_bin, counts, depth_index)))
    arrived = lax.all_to_all(
        partial.reshape(16, 1, SHARE * 128), "evt", 0, 0, tiled=True, axis_index_groups=[EVT_ORDER]
    ).reshape(16 * SHARE, 128)
    tiles = tile_of.reshape(1, 128)
    sums = pl.pallas_call(
        solve_kernel,
        out_shape=jax.ShapeDtypeStruct((16, TILE_DEV, 384), jnp.float32),
        in_specs=[vmem, vmem],
        out_specs=vmem,
        compiler_params=pltpu.CompilerParams(vmem_limit_bytes=4 << 20),
        name="solve",
    )(arrived, tiles)
    landed = lax.all_to_all(sums, "sta", 0, 0, tiled=True, axis_index_groups=[STA_ORDER])
    return pl.pallas_call(
        stack_kernel,
        out_shape=jax.ShapeDtypeStruct((TILE_DEV, 5, 2, 32), jnp.float32),
        in_specs=[vmem, vmem],
        out_specs=vmem,
        compiler_params=pltpu.CompilerParams(vmem_limit_bytes=4 << 20),
        name="stack",
    )(landed, tiles)


def solution(mesh):
    return jax.shard_map(
        body,
        mesh=mesh,
        in_specs=(
            P(None, "sta", "evt", None),
            P("sta", "evt"),
            P("sta", "evt"),
            P("sta"),
            P("sta", None),
            P(),
        ),
        out_specs=P("sta", None, None, "evt"),
        check_vma=False,
    )
```

```python
import jax
import jax.numpy as jnp
from jax import lax
from jax.experimental import pallas as pl
from jax.experimental.pallas import tpu as pltpu
from jax.sharding import PartitionSpec as P

NS = 2048
DEPTHS = 512
BAZ_BINS = 36
TILE_DEV = 4
EVT_ORDER = [11, 0, 1, 2, 3, 14, 15, 4, 5, 12, 13, 6, 7, 8, 9, 10]
STA_ORDER = [(i + 10) % 16 for i in range(16)]
STA = 8
EVT = 64
ROWS = 10
SHARE = 21
PAIRS = [(k, l) for k in range(5) for l in range(k, 5)]
WIDTHS = (512,)*4
STARTS = tuple(range(0,2048,512))
CHUNKS = len(WIDTHS)


def fit_kernel(
    traces, baz_bin, inc_bin, counts_in, depth_index, out_ref,
    data, lhs, acc, mean, picked, baz_ref, inc_ref, counts, depth_ref, sems,
):
    small = []
    for i, (source, target) in enumerate(
        ((baz_bin, baz_ref), (inc_bin, inc_ref), (counts_in, counts), (depth_index, depth_ref))
    ):
        copy = pltpu.make_async_copy(source, target, sems.at[CHUNKS + i])
        copy.start()
        small.append(copy)
    copies = []
    for n in range(CHUNKS):
        cols = pl.ds(STARTS[n], WIDTHS[n])
        copy = pltpu.make_async_copy(
            traces.at[:, :, :, cols], data.at[:, :, :, cols], sems.at[n]
        )
        copy.start()
        copies.append(copy)

    for copy in small:
        copy.wait()
    lane = lax.broadcasted_iota(jnp.int32, (STA, 128), 1)
    row = lax.broadcasted_iota(jnp.int32, (STA, 128), 0)
    baz = jnp.concatenate([baz_ref[...], baz_ref[...]], axis=1)
    inc = jnp.concatenate([inc_ref[...], inc_ref[...]], axis=1)
    phi = (baz.astype(jnp.float32) + 0.5) * (2.0 * jnp.pi / BAZ_BINS)
    tilt = (12.0 + 2.5 * (inc.astype(jnp.float32) + 0.5)) * (jnp.pi / 180.0)
    cosine = jnp.cos(phi)
    sine = jnp.sin(phi)
    cos_inc = jnp.cos(tilt)
    sin_inc = jnp.sin(tilt)
    total = jnp.zeros((STA, 128), jnp.int32)
    for s in range(STA):
        total = jnp.where(row == s, counts[s], total)
    slot = lax.axis_index("evt") * EVT + (lane & (EVT - 1))
    live = (slot < total).astype(jnp.float32)
    harm = [
        jnp.ones_like(phi),
        cosine,
        sine,
        1.0 - 2.0 * sine * sine,
        2.0 * sine * cosine,
    ]
    weighted = [h * live for h in harm]

    normal = jnp.zeros((STA, 128), jnp.float32)
    for i, (k, l) in enumerate(PAIRS):
        entry = jnp.where(lane < EVT, weighted[k] * harm[l], 0.0)
        normal = jnp.where(
            lane == row * 16 + i, jnp.sum(entry, axis=1, keepdims=True), normal
        )
    normal = jnp.sum(normal, axis=0, keepdims=True)

    quality = [sin_inc, -cos_inc * cosine, -cos_inc * sine]
    transverse = [None, sine, -cosine]
    own = [((row >> 1) == v) & ((lane >> 6) == (row & 1)) for v in range(4)]
    for comp in range(3):
        for v in range(4):
            parts = []
            for split in range(2):
                for k in range(5):
                    for base in (quality[comp], transverse[comp]):
                        if base is None:
                            parts.append(jnp.zeros((STA, 128), jnp.float32))
                            continue
                        value = weighted[k] * base
                        high = value.astype(jnp.bfloat16).astype(jnp.float32)
                        piece = high if split == 0 else value - high
                        parts.append(jnp.where(own[v], piece, 0.0))
            block = jnp.concatenate(parts, axis=0).astype(jnp.bfloat16)
            lhs[:, pl.ds((comp * 4 + v) * 128, 128)] = block

    depth = depth_ref[...]

    def pick(first, last):
        means = []
        for r in range(ROWS):
            rows = pl.ds(r * STA, STA)
            strips = [acc[rows, pl.ds(t * 128, 128)] for t in range(first, min(last + 1, 16))]
            turned = [pltpu.roll(strip, 127, 1) for strip in strips]
            for t in range(last - first):
                after = turned[t]
                if t + 1 < len(turned):
                    after = jnp.where(lane == 127, turned[t + 1], after)
                mean[r, first + t] = 0.5 * (strips[t] + after)
        for b in range(4):
            piece = depth[:, b * 128 : (b + 1) * 128]
            high, low = piece >> 7, piece & 127
            for r in range(ROWS):
                result = picked[r * 4 + b] if first else jnp.zeros((STA, 128), jnp.float32)
                for t in range(first, last):
                    result = jnp.where(
                        high == t, jnp.take_along_axis(mean[r, t], low, axis=1), result
                    )
                picked[r * 4 + b] = result

    done = 0
    for n in range(CHUNKS):
        copies[n].wait()
        cols = pl.ds(STARTS[n], WIDTHS[n])
        block = data[:, :, :, cols].reshape(3 * STA * EVT, WIDTHS[n])
        product = jnp.dot(lhs[...], block, preferred_element_type=jnp.float32)
        acc[:, cols] = product[: ROWS * STA] + product[ROWS * STA :]
        ready = STARTS[n] // 128 - 1
        if ready > done:
            pick(done, ready)
            done = ready
    pick(done, 16)
    group = lane >> 5
    turned = {}
    for r in range(ROWS):
        for b in range(4):
            whole = picked[r * 4 + b]
            turned[r, b] = pltpu.roll(whole, (r % 4) * 32, 1) if r % 4 else whole
            if r >= 8:
                turned[r + 2, b] = pltpu.roll(pltpu.roll(whole, 4, 0), (r % 4) * 32 + 64, 1)
    for b in range(4):
        for jj in range(4):
            base = EVT_ORDER.index(b * 4 + jj) * SHARE
            for g in range(3):
                value = turned[4 * g + (3 - jj) % 4, b]
                for p in range(3):
                    value = jnp.where(group == p, turned[4 * g + (p - jj) % 4, b], value)
                if g < 2:
                    out_ref[pl.ds(base + g * 8, 8), :] = value
                else:
                    out_ref[pl.ds(base + 16, 4), :] = value[0:4]
            out_ref[pl.ds(base + 20, 1), :] = normal


def solve_kernel(parts_ref, tile_ref, out_ref):
    lane = lax.broadcasted_iota(jnp.int32, (STA, 128), 1)
    row = lax.broadcasted_iota(jnp.int32, (STA, 128), 0)
    total = []
    for start, size in ((0, 8), (8, 8), (16, 5)):
        pieces = [parts_ref[pl.ds(j * SHARE + start, size), :] for j in range(16)]
        while len(pieces) > 1:
            pieces = [x + y for x, y in zip(pieces[::2], pieces[1::2])]
        total.append(pieces[0])
    normal = jnp.broadcast_to(total[2][4:5], (STA, 128))
    normal = jnp.take_along_axis(normal, row * 16 + (lane & 15), axis=1)
    back = lax.rem(4 - lax.rem(lax.axis_index("evt"), 4), 4) * 32
    folded = pltpu.roll(total[2][0:4], back, 1)
    mine = [
        pltpu.roll(total[0], back, 1),
        pltpu.roll(total[1], back, 1),
        jnp.concatenate([folded, pltpu.roll(folded, 64, 1)], axis=0),
    ]
    entry = {}
    for i, (k, l) in enumerate(PAIRS):
        value = jnp.broadcast_to(normal[:, i : i + 1], (STA, 128))
        entry[k, l] = value + 1.0 if k == l else value
    right = []
    for k in range(5):
        right.append(pltpu.roll(mine[k // 2], 64, 1) if k % 2 else mine[k // 2])
    inverse = []
    for k in range(5):
        inv = 1.0 / entry[k, k]
        inverse.append(inv)
        for l in range(k + 1, 5):
            factor = entry[k, l] * inv
            for m in range(l, 5):
                entry[l, m] = entry[l, m] - factor * entry[k, m]
            right[l] = right[l] - factor * right[k]
    solved = [None] * 5
    for k in reversed(range(5)):
        value = right[k]
        for l in range(k + 1, 5):
            value = value - entry[k, l] * solved[l]
        solved[k] = value * inverse[k]
    low = lane < 64
    joined = jnp.concatenate(
        [
            jnp.where(low, solved[0], pltpu.roll(solved[1], 64, 1)),
            jnp.where(low, solved[2], pltpu.roll(solved[3], 64, 1)),
            jnp.where(low, solved[4], 0.0),
        ],
        axis=1,
    )
    shift = lax.rem(128 - lax.axis_index("sta") * STA, 128)
    local = pltpu.roll(jnp.broadcast_to(tile_ref[...], (8, 128)), shift, 1)[0:1, 0:STA]
    ids = lax.broadcasted_iota(jnp.int32, (64, STA), 0)
    onehot = (jnp.broadcast_to(local, (64, STA)) == ids).astype(jnp.float32)
    sums = jnp.dot(
        onehot, joined, precision=lax.Precision.HIGHEST, preferred_element_type=jnp.float32
    )
    for i in range(16):
        out_ref[STA_ORDER.index(i)] = sums[i * TILE_DEV : (i + 1) * TILE_DEV]


def stack_kernel(parts_ref, tile_ref, out_ref):
    sums = jnp.sum(parts_ref[...], axis=0)
    own = lax.axis_index("sta") * TILE_DEV + lax.broadcasted_iota(jnp.int32, (TILE_DEV, 128), 0)
    match = (jnp.broadcast_to(tile_ref[...], (TILE_DEV, 128)) == own).astype(jnp.float32)
    members = jnp.sum(match, axis=1, keepdims=True)
    scale = 1.0 / jnp.maximum(members, 1.0)
    for k in range(5):
        for c in range(2):
            out_ref[:, k, c, :] = sums[:, k * 64 + c * 32 : k * 64 + c * 32 + 32] * scale


def body(traces, baz_bin, inc_bin, counts, depth_index, tile_of):
    vmem = pl.BlockSpec(memory_space=pltpu.VMEM)
    partial = pl.pallas_call(
        fit_kernel,
        out_shape=jax.ShapeDtypeStruct((16 * SHARE, 128), jnp.float32),
        in_specs=[pl.BlockSpec(memory_space=pltpu.HBM)] * 5,
        out_specs=vmem,
        scratch_shapes=[
            pltpu.VMEM((3, STA, EVT, NS), jnp.bfloat16),
            pltpu.VMEM((2 * ROWS * STA, 3 * STA * EVT), jnp.bfloat16),
            pltpu.VMEM((ROWS * STA, NS), jnp.float32),
            pltpu.VMEM((ROWS, 16, STA, 128), jnp.float32),
            pltpu.VMEM((ROWS * 4, STA, 128), jnp.float32),
            pltpu.VMEM((STA, EVT), jnp.int32),
            pltpu.VMEM((STA, EVT), jnp.int32),
            pltpu.SMEM((STA,), jnp.int32),
            pltpu.VMEM((STA, DEPTHS), jnp.int32),
            pltpu.SemaphoreType.DMA((CHUNKS + 4,)),
        ],
        compiler_params=pltpu.CompilerParams(vmem_limit_bytes=16 << 20),
        name="fit",
    )(*(pltpu.with_memory_space_constraint(x, pltpu.HBM) for x in (traces, baz_bin, inc_bin, counts, depth_index)))
    arrived = lax.all_to_all(
        partial.reshape(16, 1, SHARE * 128), "evt", 0, 0, tiled=True, axis_index_groups=[EVT_ORDER]
    ).reshape(16 * SHARE, 128)
    tiles = tile_of.reshape(1, 128)
    sums = pl.pallas_call(
        solve_kernel,
        out_shape=jax.ShapeDtypeStruct((16, TILE_DEV, 384), jnp.float32),
        in_specs=[vmem, vmem],
        out_specs=vmem,
        compiler_params=pltpu.CompilerParams(vmem_limit_bytes=4 << 20),
        name="solve",
    )(arrived, tiles)
    landed = lax.all_to_all(sums, "sta", 0, 0, tiled=True, axis_index_groups=[STA_ORDER])
    return pl.pallas_call(
        stack_kernel,
        out_shape=jax.ShapeDtypeStruct((TILE_DEV, 5, 2, 32), jnp.float32),
        in_specs=[vmem, vmem],
        out_specs=vmem,
        compiler_params=pltpu.CompilerParams(vmem_limit_bytes=4 << 20),
        name="stack",
    )(landed, tiles)


def solution(mesh):
    return jax.shard_map(
        body,
        mesh=mesh,
        in_specs=(
            P(None, "sta", "evt", None),
            P("sta", "evt"),
            P("sta", "evt"),
            P("sta"),
            P("sta", None),
            P(),
        ),
        out_specs=P("sta", None, None, "evt"),
        check_vma=False,
    )
```
